128 devices in a mesh: tm: 16 (over z, x_hi, core), space: 8 (over x_lo, y).
Axes of the slice: x: 4 (x_hi: 2, x_lo: 2; x = x_hi * 2 + x_lo), y: 4, z: 4, core: 2. Of those that a mesh axis runs over, the one named last changes fastest.
Arguments:
- solution: float32 [512, 384, 384], P('tm', 'space'), may hold values from -6 to 6
- residual: float32 [512, 384, 384], P('tm', 'space'), may hold values from -6 to 6
- direction: float32 [512, 384, 384], P('tm', 'space'), may hold values from -6 to 6
- reaction: float32 [512, 384, 384], P('tm', 'space'), may hold values from 0.1 to 2
- time_bands: float32 [2, 4, 512], replicated, may hold values from -0.25 to 1.1, as said below
- space_bands: float32 [2, 4, 384], replicated, may hold values from -0.25 to 1.1, as said below
- time_basis: float32 [512, 512], replicated, may hold values from -0.25 to 0.25
- space_basis: float32 [384, 384], replicated, may hold values from -0.3125 to 0.3125
- time_eigen: float32 [512], replicated, may hold values from 0.1 to 1
- space_eigen: float32 [384], replicated, may hold values from 0.1 to 1
Outputs:
- new_solution: float32 [512, 384, 384], P('tm', 'space')
- new_residual: float32 [512, 384, 384], P('tm', 'space')
- new_direction: float32 [512, 384, 384], P('tm', 'space')
The draws below stay inside these ranges and needn't reach their ends.
Inputs may be any that keep to these rules, and one draw needn't show every extreme that they name: `time_bands`: each of the two matrices is symmetric with every diagonal entry larger than the sum of the magnitudes of the other entries of its row. `space_bands`: each of the two matrices is symmetric with every diagonal entry larger than the sum of the magnitudes of the other entries of its row.
All inputs are finite; a program needn't handle non-finite values.
Results may differ from the reference program's by a relative error of at most 0.000051.
Values sent between devices are 32-bit elements; how exact they have to be, the bound alone decides.
A program may use at most 128 MiB of HBM per device.

```python
import math
import jax
import jax.numpy as jnp
from jax import lax

NT = 512
NS = 384


def band_table(key, length):
    subkeys = jax.random.split(key, 8)
    tables = []
    for matrix_index in range(2):
        diagonal = jax.random.uniform(subkeys[4 * matrix_index], (length,), jnp.float32, 0.9, 1.1)
        near_band = jax.random.uniform(subkeys[4 * matrix_index + 1], (length,), jnp.float32, -0.25, 0.25)
        middle_band = jax.random.uniform(subkeys[4 * matrix_index + 2], (length,), jnp.float32, -0.12, 0.12)
        outer_band = jax.random.uniform(subkeys[4 * matrix_index + 3], (length,), jnp.float32, -0.05, 0.05)
        tables.append(jnp.stack([diagonal, near_band, middle_band, outer_band]))
    return jnp.stack(tables)


def draw_time_bands(key, part):
    return band_table(jax.random.fold_in(key, 11), NT)


def draw_space_bands(key, part):
    return band_table(jax.random.fold_in(key, 23), NS)


def shard_levels(own_key, shape, pieces, smallest, top_value):
    loudness, own = 1.0, jax.random.fold_in(own_key, 6)
    for axis_at, parts in pieces:
        draws = jnp.exp(jax.random.uniform(jax.random.fold_in(own, axis_at), (parts,), jnp.float32, smallest / len(pieces), top_value / len(pieces)))
        loudness = loudness * jnp.repeat(draws, shape[axis_at] // parts).reshape([-1 if axis == axis_at else 1 for axis in range(len(shape))])
    return loudness


def centred(key, shape, width, bound, pieces=(), kind=jnp.bfloat16):
    entries = width * jax.random.normal(key, shape, jnp.float32)
    if pieces:
        entries = entries * shard_levels(key, shape, pieces, -0.22, 0.18)
    return jnp.clip(entries, -bound, bound).astype(kind)


def setup_inputs(seed: int = 0) -> dict:
    key_list = jax.random.split(jax.random.key(seed), 11)
    return {
        "solution": centred(key_list[0], (NT, NS, NS), 1.0, 6.0, ((0, 16), (1, 8)), jnp.float32),
        "residual": centred(key_list[1], (NT, NS, NS), 1.0, 6.0, ((0, 16), (1, 8)), jnp.float32),
        "direction": centred(key_list[2], (NT, NS, NS), 1.0, 6.0, ((0, 16), (1, 8)), jnp.float32),
        "reaction": jnp.clip(jnp.exp(math.log(2.0) - 2.9957323 * jax.random.uniform(key_list[3], (NT, NS, NS), jnp.float32) ** shard_levels(key_list[3], (NT, NS, NS), ((0, 16), (1, 8)), -0.2, 0.2)), 0.1, 2.0),
        "time_bands": draw_time_bands(jax.random.fold_in(key_list[10], 71), 0),
        "space_bands": draw_space_bands(jax.random.fold_in(key_list[10], 71), 0),
        "time_basis": centred(key_list[6], (NT, NT), NT ** -0.5, 0.25, (), jnp.float32),
        "space_basis": centred(key_list[7], (NS, NS), NS ** -0.5, 0.3125, (), jnp.float32),
        "time_eigen": jnp.clip(jnp.exp(jax.random.uniform(key_list[8], (NT,), jnp.float32, math.log(0.1), math.log(1.0))), 0.1, 1.0),
        "space_eigen": jnp.clip(jnp.exp(jax.random.uniform(key_list[9], (NS,), jnp.float32, math.log(0.1), math.log(1.0))), 0.1, 1.0),
    }


highest = lax.Precision.HIGHEST


def band_apply(extended, band_rows, dimension):
    length = extended.shape[dimension] - 6
    target_shape = [1] * extended.ndim
    target_shape[dimension] = length

    def coefficient(which_row, first_row):
        return lax.slice_in_dim(band_rows[which_row], first_row, first_row + length).reshape(target_shape)

    def window(first_row):
        return lax.slice_in_dim(extended, first_row, first_row + length, axis=dimension)

    result = coefficient(0, 3) * window(3)
    for offset in (1, 2, 3):
        result = result + coefficient(offset, 3) * window(3 + offset) + coefficient(offset, 3 - offset) * window(3 - offset)
    return result


def pad_along(values, dimension):
    widths = [(0, 0)] * values.ndim
    widths[dimension] = (3, 3)
    return jnp.pad(values, widths)


def apply_operator(direction, reaction, time_bands, space_bands):
    padded_time = jnp.pad(time_bands, ((0, 0), (0, 0), (3, 3)))
    padded_space = jnp.pad(space_bands, ((0, 0), (0, 0), (3, 3)))
    extended = pad_along(direction, 2)
    mass_y = band_apply(extended, padded_space[1], 2)
    stiff_y = band_apply(extended, padded_space[0], 2)
    mass_xy = band_apply(pad_along(mass_y, 1), padded_space[1], 1)
    stiff_x = band_apply(pad_along(mass_y, 1), padded_space[0], 1)
    stiff_yx = band_apply(pad_along(stiff_y, 1), padded_space[1], 1)
    temporal = band_apply(pad_along(mass_xy, 0), padded_time[0], 0) + band_apply(pad_along(stiff_x + stiff_yx, 0), padded_time[1], 0)
    return temporal + reaction * direction


def forward_transform(values, time_basis, space_basis):
    along_y = jnp.einsum('txk,ka->txa', values, space_basis, precision=highest)
    along_x = jnp.einsum('tjy,jb->tby', along_y, space_basis, precision=highest)
    return jnp.einsum('ixy,ia->axy', along_x, time_basis, precision=highest)


def inverse_transform(spectral, time_basis, space_basis):
    along_t = jnp.einsum('axy,ia->ixy', spectral, time_basis, precision=highest)
    along_x = jnp.einsum('tby,jb->tjy', along_t, space_basis, precision=highest)
    return jnp.einsum('txa,ka->txk', along_x, space_basis, precision=highest)


def reference(solution, residual, direction, reaction, time_bands, space_bands, time_basis, space_basis, time_eigen, space_eigen):
    image = apply_operator(direction, reaction, time_bands, space_bands)
    eigen_sum = time_eigen[:, None, None] + space_eigen[:, None] + space_eigen[None, :]
    first_hat = forward_transform(residual, time_basis, space_basis)
    norm_old = jnp.sum(first_hat * (first_hat / eigen_sum))
    curvature = jnp.sum(direction * image)
    step_size = norm_old / curvature
    new_solution = solution + step_size * direction
    new_residual = residual - step_size * image
    new_hat = forward_transform(new_residual, time_basis, space_basis)
    spectral = new_hat / eigen_sum
    norm_new = jnp.sum(new_hat * spectral)
    precond = inverse_transform(spectral, time_basis, space_basis)
    new_direction = precond + (norm_new / norm_old) * direction
    return new_solution, new_residual, new_direction
```

```python
import jax
import jax.numpy as jnp
from jax import lax
from jax.experimental import pallas as pl
from jax.experimental.pallas import tpu as pltpu
from jax.sharding import PartitionSpec as P

F32 = jnp.float32
BF16 = jnp.bfloat16
MESH = pl.DeviceIdType.MESH
ROWS = 36


def split(x):
    high = x.astype(BF16)
    return high, (x - high.astype(F32)).astype(BF16)


def dot(a, b, ca=1, cb=0):
    return lax.dot_general(a, b, (((ca,), (cb,)), ((), ())), preferred_element_type=F32)


def position():
    tm = lax.axis_index("tm")
    sp = lax.axis_index("space")
    return tm // 4, (tm // 2) % 2 * 2 + sp // 4, sp % 4, tm % 2


def device(z, x, y, c):
    return z * 4 + (x // 2) * 2 + c, (x % 2) * 4 + y


def partner(i, where):
    z, x, y, c = where
    a, b, e, d = i % 4, (i // 4) % 4, (i // 16) % 4, i // 64
    return device((z + a) % 4, (x + a + b) % 4, (y + a + b + e) % 4, (c + d + a) % 2)


def swap_lanes(pieces):
    lane = lax.broadcasted_iota(jnp.int32, (8, 128), 1)
    for bit in (1, 2, 4):
        low = (lane & bit) == 0
        moved = list(pieces)
        for p in range(8):
            if p & bit == 0:
                a, b = pieces[p], pieces[p | bit]
                moved[p] = jnp.where(low, a, pltpu.roll(b, bit, 1))
                moved[p | bit] = jnp.where(low, pltpu.roll(a, 128 - bit, 1), b)
        pieces = moved
    return pieces


def to_lines(chunks, lines):
    def body(i, carry):
        k, h = i // 6, i % 6
        for tau in range(2):
            for top in range(2):
                row = k * 12 + tau * 6 + h
                got = [
                    chunks[pl.ds((top * 8 + p) * 8 * ROWS + row, 8, stride=ROWS), :]
                    for p in range(8)
                ]
                base = pl.multiple_of(k * 384 + h * 64, 64)
                lanes = slice((top * 2 + tau) * 128, (top * 2 + tau + 1) * 128)
                for x8, piece in enumerate(swap_lanes(got)):
                    lines[pl.ds(base + x8 * 8, 8), lanes] = piece
        return carry

    lax.fori_loop(0, 18, body, 0)


def to_chunks(lines, chunks):
    def body(i, carry):
        k, h = i // 6, i % 6
        for tau in range(2):
            for top in range(2):
                row = k * 12 + tau * 6 + h
                base = pl.multiple_of(k * 384 + h * 64, 64)
                lanes = slice((top * 2 + tau) * 128, (top * 2 + tau + 1) * 128)
                got = [lines[pl.ds(base + x8 * 8, 8), lanes] for x8 in range(8)]
                for p, piece in enumerate(swap_lanes(got)):
                    chunks[pl.ds((top * 8 + p) * 8 * ROWS + row, 8, stride=ROWS), :] = piece
        return carry

    lax.fori_loop(0, 18, body, 0)


def forward_y(field, left, chunks):
    def body(i, carry):
        tau, h = i // 3, (i % 3) * 2
        v = field[pl.ds(pl.multiple_of(tau * 16, 16), 16), pl.ds(pl.multiple_of(h * 8, 16), 16), :]
        high, low = split(
            jnp.concatenate([v[:, 0:8].reshape(128, 384), v[:, 8:16].reshape(128, 384)], axis=0)
        )
        out = dot(left[...], jnp.concatenate([high, low, high], axis=1), 1, 1)
        for k in range(3):
            for j in range(2):
                chunks[pl.ds(k * 12 + tau * 6 + h + j, 128, stride=ROWS), :] = out[
                    k * 128 : (k + 1) * 128, j * 128 : (j + 1) * 128
                ]
        return carry

    lax.fori_loop(0, 6, body, 0)


def tripled(ref, values):
    high, low = split(values)
    width = values.shape[1]
    ref[:, 0:width] = high
    ref[:, width : 2 * width] = high
    ref[:, 2 * width : 3 * width] = low


def stacked(values):
    high, low = split(values)
    return jnp.concatenate([high, low, high], axis=0)


def forward_tx(lines, time_high, time_low, left_x, out):
    def body(k, carry):
        rows = pl.ds(pl.multiple_of(k * 384, 384), 384)
        high, low = split(lines[rows, :])
        mid = dot(high, time_high[...]) + dot(high, time_low[...]) + dot(low, time_high[...])
        out[rows, :] = dot(left_x[...], stacked(mid))
        return carry

    lax.fori_loop(0, 3, body, 0)


def send_all(where, copy_to):
    def body(i, carry):
        copy_to(*partner(i, where)).start()
        return carry

    lax.fori_loop(1, 128, body, 0)


def stencil(ext, reac, ycoef, xcoef, tcoef, mass, stiff, mixed, rest, image):
    def along_y(t, carry):
        for part in range(4):
            rows = slice(part * 16, part * 16 + 16)
            v = ext[t, rows, :]
            m = ycoef[3:4, :] * v
            s = ycoef[10:11, :] * v
            for off in (-3, -2, -1, 1, 2, 3):
                moved = pltpu.roll(v, (-off) % 384, 1)
                m = m + ycoef[3 + off : 4 + off, :] * moved
                s = s + ycoef[10 + off : 11 + off, :] * moved
            for c in range(3):
                mass[t, c, rows, :] = m[:, c * 128 : (c + 1) * 128]
                stiff[t, c, rows, :] = s[:, c * 128 : (c + 1) * 128]
        return carry

    lax.fori_loop(0, 38, along_y, 0)

    for i in range(6):
        first = i * 8
        ms = [xcoef[j, first : first + 8, :] for j in range(7)]
        ks = [xcoef[7 + j, first : first + 8, :] for j in range(7)]

        def along_x(t, carry):
            for c in range(3):
                m = [mass[t, c, 5 + j + first : 13 + j + first, :] for j in range(7)]
                s = [stiff[t, c, 5 + j + first : 13 + j + first, :] for j in range(7)]
                a = ms[0] * m[0]
                b = ks[0] * m[0] + ms[0] * s[0]
                for j in range(1, 7):
                    a = a + ms[j] * m[j]
                    b = b + (ks[j] * m[j] + ms[j] * s[j])
                mixed[t, c, first : first + 8, :] = a
                rest[t, c, first : first + 8, :] = b
            return carry

        lax.fori_loop(0, 38, along_x, 0)

    def along_t(t, total):
        kt = [tcoef[j * 32 + t] for j in range(7)]
        mt = [tcoef[(7 + j) * 32 + t] for j in range(7)]
        for c in range(3):
            lanes = slice(c * 128, c * 128 + 128)
            for i in range(6):
                rows = slice(i * 8, i * 8 + 8)
                own = ext[t + 3, 8 + i * 8 : 16 + i * 8, lanes]
                value = reac[t, rows, lanes] * own
                for j in range(7):
                    value = value + (
                        kt[j] * mixed[t + j, c, rows, :] + mt[j] * rest[t + j, c, rows, :]
                    )
                image[t, rows, lanes] = value
                total = total + own * value
        return total

    return lax.fori_loop(0, 32, along_t, jnp.zeros((8, 128), F32))


def whole(x):
    return jnp.sum(jnp.sum(x, axis=1, keepdims=True), axis=0, keepdims=True)


def main_kernel(
    r_h, d_h, reac_h, s_h, sp_h, tp_h, base_h, yc_h, xc_h, tcoef, seig,
    img_h, back_h, scal_o,
    rv, ext, reac, image, s_v, sp_v, tp_v, base_v, yc_v, xc_v,
    left_y, left_x, left_xi, time_high, time_low,
    send1, send2, send3, recv1, recv2, lines, hat_r, hat_i,
    mass, stiff, mixed, rest, red1s, red1, red2s, red2,
    local, halo_s, halo_r, out_sem, send_sem, recv_sem,
):
    where = position()
    tm = lax.axis_index("tm")
    sp = lax.axis_index("space")
    me = tm * 8 + sp
    loads = [
        pltpu.make_async_copy(src, dst, local.at[n])
        for n, (src, dst) in enumerate(
            [
                (d_h, ext.at[3:35, 8:56]), (s_h, s_v), (r_h, rv), (reac_h, reac),
                (sp_h, sp_v), (tp_h, tp_v), (base_h, base_v), (yc_h, yc_v), (xc_h, xc_v),
            ]
        )
    ]
    for load in loads:
        load.start()

    barrier = pltpu.get_barrier_semaphore()

    def greet(i, carry):
        pl.semaphore_signal(barrier, inc=1, device_id=partner(i, where), device_id_type=MESH)
        return carry

    lax.fori_loop(1, 128, greet, 0)
    loads[1].wait()
    tripled(left_y, s_v[...].T)
    loads[0].wait()
    pl.semaphore_wait(barrier, 127)

    halos = []
    for dt, src_t, dst_t in ((-1, slice(3, 6), slice(35, 38)), (0, slice(3, 35), slice(3, 35)), (1, slice(32, 35), slice(0, 3))):
        for dx, src_x, dst_x in ((-1, slice(8, 16), slice(56, 64)), (0, slice(8, 56), slice(8, 56)), (1, slice(48, 56), slice(0, 8))):
            if dt or dx:
                n = len(halos)
                halos.append(
                    pltpu.make_async_remote_copy(
                        src_ref=ext.at[src_t, src_x],
                        dst_ref=ext.at[dst_t, dst_x],
                        send_sem=halo_s.at[n],
                        recv_sem=halo_r.at[n],
                        device_id=((tm + 16 + dt) % 16, (sp + 8 + dx) % 8),
                        device_id_type=MESH,
                    )
                )
    for halo in halos:
        halo.start()

    def chunk(ref, d):
        return ref.at[pl.ds(d * ROWS, ROWS)]

    def exchange(n, src, dst):
        def copy_to(t, s):
            return pltpu.make_async_remote_copy(
                src_ref=chunk(src, t * 8 + s),
                dst_ref=chunk(dst, me),
                send_sem=send_sem.at[n],
                recv_sem=recv_sem.at[n],
                device_id=(t, s),
                device_id_type=MESH,
            )

        send_all(where, copy_to)

    def finish(n, src, dst, rows):
        return pltpu.make_async_remote_copy(
            src_ref=src.at[pl.ds(0, 127 * rows)],
            dst_ref=dst.at[pl.ds(0, 127 * rows)],
            send_sem=send_sem.at[n],
            recv_sem=recv_sem.at[n],
            device_id=(tm, sp),
            device_id_type=MESH,
        )

    def own_chunk(src, dst):
        dst[pl.ds(me * ROWS, ROWS), :] = src[pl.ds(me * ROWS, ROWS), :]

    loads[2].wait()
    forward_y(rv, left_y, send1)
    exchange(0, send1, recv1)
    own_chunk(send1, recv1)

    for load in loads[3:]:
        load.wait()
    for halo in halos:
        halo.wait()
    curve = stencil(ext, reac, yc_v, xc_v, tcoef, mass, stiff, mixed, rest, image)
    store_image = pltpu.make_async_copy(image, img_h, out_sem.at[0])
    store_image.start()
    forward_y(image, left_y, send2)
    exchange(1, send2, recv2)
    own_chunk(send2, recv2)

    tripled(left_x, sp_v[...].T)
    tripled(left_xi, sp_v[...])
    high, low = split(tp_v[...])
    time_high[...] = high
    time_low[...] = low

    finish(0, send1, recv1, ROWS).wait()
    to_lines(recv1, lines)
    forward_tx(lines, time_high, time_low, left_x, hat_r)

    def eigen(k):
        return base_v[...] + seig[k * 128 + me]

    def old_part(k, total):
        v = hat_r[pl.ds(pl.multiple_of(k * 384, 384), 384), :]
        return total + jnp.sum((v * (v / eigen(k))).reshape(48, 8, 512), axis=0)

    old = lax.fori_loop(0, 3, old_part, jnp.zeros((8, 512), F32))
    old = old[:, 0:128] + old[:, 128:256] + old[:, 256:384] + old[:, 384:512]

    def share(n, mine, every, rows):
        def copy_to(t, s):
            return pltpu.make_async_remote_copy(
                src_ref=mine,
                dst_ref=every.at[pl.ds(me * rows, rows)],
                send_sem=send_sem.at[n],
                recv_sem=recv_sem.at[n],
                device_id=(t, s),
                device_id_type=MESH,
            )

        send_all(where, copy_to)
        every[pl.ds(me * rows, rows), :] = mine[...]

    red1s[0:1, :] = jnp.sum(old, axis=0, keepdims=True)
    red1s[1:2, :] = jnp.sum(curve, axis=0, keepdims=True)
    share(3, red1s, red1, 2)

    finish(1, send2, recv2, ROWS).wait()
    to_lines(recv2, lines)
    forward_tx(lines, time_high, time_low, left_x, hat_i)

    finish(3, red1, red1, 2).wait()
    every = red1[...]
    even = lax.broadcasted_iota(jnp.int32, (256, 128), 0) % 2 == 0
    norm_old = whole(jnp.where(even, every, 0.0))
    step = norm_old / whole(jnp.where(even, 0.0, every))

    def inverse_part(k, total):
        rows = pl.ds(pl.multiple_of(k * 384, 384), 384)
        v = hat_r[rows, :] - step * hat_i[rows, :]
        g = v / eigen(k)
        high, low = split(dot(left_xi[...], stacked(g)))
        lines[rows, :] = (
            dot(high, time_high[...], 1, 1)
            + dot(high, time_low[...], 1, 1)
            + dot(low, time_high[...], 1, 1)
        )
        return total + jnp.sum((v * g).reshape(48, 8, 512), axis=0)

    new = lax.fori_loop(0, 3, inverse_part, jnp.zeros((8, 512), F32))
    to_chunks(lines, send3)
    exchange(2, send3, back_h)
    own = pltpu.make_async_copy(chunk(send3, me), chunk(back_h, me), out_sem.at[1])
    own.start()

    new = new[:, 0:128] + new[:, 128:256] + new[:, 256:384] + new[:, 384:512]
    red2s[...] = jnp.sum(new, axis=0, keepdims=True)
    share(4, red2s, red2, 1)
    finish(4, red2, red2, 1).wait()
    norm_new = whole(red2[...])
    row = lax.broadcasted_iota(jnp.int32, (8, 128), 0)
    scal_o[...] = jnp.where(row == 0, step, norm_new / norm_old)

    store_image.wait()
    own.wait()
    finish(2, send3, back_h, ROWS).wait()


def last_kernel(
    back_h, s_h, d_h, sol_h, r_h, img_h, scal,
    new_sol, new_res, new_dir,
    back, s_v, left, d_v, sol_v, r_v, img_v, ns_v, nr_v, nd_v, in_sem, out_sem,
):
    start = [pltpu.make_async_copy(s_h, s_v, in_sem.at[0]), pltpu.make_async_copy(back_h, back, in_sem.at[1])]
    halves = []
    for half in range(2):
        t = slice(half * 16, half * 16 + 16)
        halves.append(
            [
                pltpu.make_async_copy(src.at[t], dst.at[t], in_sem.at[2 + half * 4 + n])
                for n, (src, dst) in enumerate(((d_h, d_v), (sol_h, sol_v), (r_h, r_v), (img_h, img_v)))
            ]
        )
    for copy in start + halves[0] + halves[1]:
        copy.start()
    start[0].wait()
    tripled(left, s_v[...])
    start[1].wait()
    step = scal[0:1, 0:1]
    ratio = scal[1:2, 0:1]
    stores = []
    for tau in range(2):
        t = slice(tau * 16, tau * 16 + 16)
        for copy in halves[tau]:
            copy.wait()

        def body(i, carry):
            h = i * 2
            parts = []
            for j in range(2):
                parts.append(
                    jnp.concatenate(
                        [back[pl.ds(k * 12 + tau * 6 + h + j, 128, stride=ROWS), :] for k in range(3)], axis=0
                    )
                )
            out = dot(left[...], stacked(jnp.concatenate(parts, axis=1))).T
            for j in range(2):
                x = pl.ds(pl.multiple_of((h + j) * 8, 8), 8)
                d = d_v[t, x, :]
                nd_v[t, x, :] = out[j * 128 : (j + 1) * 128, :].reshape(16, 8, 384) + ratio.reshape(1, 1, 1) * d
                ns_v[t, x, :] = sol_v[t, x, :] + step.reshape(1, 1, 1) * d
                nr_v[t, x, :] = r_v[t, x, :] - step.reshape(1, 1, 1) * img_v[t, x, :]
            return carry

        lax.fori_loop(0, 3, body, 0)
        for n, (src, dst) in enumerate(((ns_v, new_sol), (nr_v, new_res), (nd_v, new_dir))):
            stores.append(pltpu.make_async_copy(src.at[t], dst.at[t], out_sem.at[tau * 3 + n]))
            stores[-1].start()
    for store in stores:
        store.wait()


def band_lines(table):
    n = table.shape[1]
    lines = []
    for off in range(-3, 4):
        size = abs(off)
        zeros = jnp.zeros((size,), F32)
        kept = table[size, : n - size]
        lines.append(jnp.concatenate([zeros, kept] if off < 0 else [kept, zeros]))
    return jnp.stack(lines)


ANY = pl.BlockSpec(memory_space=pl.ANY)
VMEM = pl.BlockSpec(memory_space=pltpu.VMEM)
SMEM = pl.BlockSpec(memory_space=pltpu.SMEM)


def per_device(solution, residual, direction, reaction, time_bands, space_bands, time_basis, space_basis, time_eigen, space_eigen):
    tm = lax.axis_index("tm")
    sp = lax.axis_index("space")
    space_lines = jnp.concatenate([band_lines(space_bands[1]), band_lines(space_bands[0])])
    time_lines = jnp.concatenate([band_lines(time_bands[0]), band_lines(time_bands[1])])
    x_lines = lax.dynamic_slice_in_dim(space_lines, sp * 48, 48, 1)
    t_lines = lax.dynamic_slice_in_dim(time_lines, tm * 32, 32, 1).reshape(-1)
    x_lines = jnp.broadcast_to(x_lines[:, :, None], (14, 48, 128))
    basis_x = space_basis.reshape(8, 6, 8, 384).transpose(1, 2, 0, 3).reshape(384, 384)
    basis_t = time_basis.reshape(2, 8, 2, 16, 512).transpose(0, 2, 3, 1, 4).reshape(512, 512)
    base = space_eigen[:, None] + time_eigen[None, :]
    block = (32, 48, 384)
    chunks = (128 * ROWS, 128)
    v = pltpu.VMEM
    dma = pltpu.SemaphoreType.DMA
    image, back, scal = pl.pallas_call(
        main_kernel,
        out_shape=(
            jax.ShapeDtypeStruct(block, F32),
            jax.ShapeDtypeStruct(chunks, F32),
            jax.ShapeDtypeStruct((8, 128), F32),
        ),
        in_specs=[ANY] * 9 + [SMEM] * 2,
        out_specs=(ANY, ANY, VMEM),
        scratch_shapes=[
            v(block, F32), v((38, 64, 384), F32), v(block, F32), v(block, F32),
            v((384, 384), F32), v((384, 384), F32), v((512, 512), F32), v((384, 512), F32),
            v((14, 384), F32), v((14, 48, 128), F32),
            v((384, 1152), BF16), v((384, 1152), BF16), v((384, 1152), BF16),
            v((512, 512), BF16), v((512, 512), BF16),
            v(chunks, F32), v(chunks, F32), v(chunks, F32), v(chunks, F32), v(chunks, F32),
            v((1152, 512), F32), v((1152, 512), F32), v((1152, 512), F32),
            v((38, 3, 64, 128), F32), v((38, 3, 64, 128), F32),
            v((38, 3, 48, 128), F32), v((38, 3, 48, 128), F32),
            v((2, 128), F32), v((256, 128), F32), v((1, 128), F32), v((128, 128), F32),
            dma((9,)), dma((8,)), dma((8,)), dma((2,)), dma((5,)), dma((5,)),
        ],
        compiler_params=pltpu.CompilerParams(
            collective_id=0, has_side_effects=True, vmem_limit_bytes=62 * 2**20
        ),
    )(residual, direction, reaction, space_basis, basis_x, basis_t, base, space_lines, x_lines, t_lines, space_eigen)
    return pl.pallas_call(
        last_kernel,
        out_shape=(jax.ShapeDtypeStruct(block, F32),) * 3,
        in_specs=[ANY] * 6 + [VMEM],
        out_specs=(ANY,) * 3,
        scratch_shapes=[
            v(chunks, F32), v((384, 384), F32), v((384, 1152), BF16),
            *[v(block, F32) for _ in range(7)],
            dma((10,)), dma((6,)),
        ],
        compiler_params=pltpu.CompilerParams(vmem_limit_bytes=48 * 2**20),
    )(back, space_basis, direction, solution, residual, image, scal)


def solution(mesh):
    field = P("tm", "space", None)
    return jax.shard_map(
        per_device,
        mesh=mesh,
        in_specs=(field,) * 4 + (P(),) * 6,
        out_specs=(field,) * 3,
        check_vma=False,
    )
```

```python
import jax
import jax.numpy as jnp
from jax import lax
from jax.experimental import pallas as pl
from jax.experimental.pallas import tpu as pltpu
from jax.sharding import PartitionSpec as P

F32 = jnp.float32
BF16 = jnp.bfloat16
MESH = pl.DeviceIdType.MESH
ROWS = 36


def split(x):
    high = x.astype(BF16)
    return high, (x - high.astype(F32)).astype(BF16)


def dot(a, b, ca=1, cb=0):
    return lax.dot_general(a, b, (((ca,), (cb,)), ((), ())), preferred_element_type=F32)


def position():
    tm = lax.axis_index("tm")
    sp = lax.axis_index("space")
    return tm // 4, (tm // 2) % 2 * 2 + sp // 4, sp % 4, tm % 2


def device(z, x, y, c):
    return z * 4 + (x // 2) * 2 + c, (x % 2) * 4 + y


def partner(i, where):
    z, x, y, c = where
    a, b, e, d = i % 4, (i // 4) % 4, (i // 16) % 4, i // 64
    return device((z + a) % 4, (x + a + b) % 4, (y + a + b + e) % 4, (c + d + a) % 2)


def swap_lanes(pieces):
    lane = lax.broadcasted_iota(jnp.int32, (8, 128), 1)
    for bit in (1, 2, 4):
        low = (lane & bit) == 0
        moved = list(pieces)
        for p in range(8):
            if p & bit == 0:
                a, b = pieces[p], pieces[p | bit]
                moved[p] = jnp.where(low, a, pltpu.roll(b, bit, 1))
                moved[p | bit] = jnp.where(low, pltpu.roll(a, 128 - bit, 1), b)
        pieces = moved
    return pieces


def to_lines(chunks, k, lines):
    def body(h, carry):
        for tau in range(2):
            for top in range(2):
                row = k * 12 + tau * 6 + h
                got = [
                    chunks[pl.ds((top * 8 + p) * 8 * ROWS + row, 8, stride=ROWS), :]
                    for p in range(8)
                ]
                base = pl.multiple_of(h * 64, 64)
                lanes = slice((top * 2 + tau) * 128, (top * 2 + tau + 1) * 128)
                for x8, piece in enumerate(swap_lanes(got)):
                    lines[pl.ds(base + x8 * 8, 8), lanes] = piece
        return carry

    lax.fori_loop(0, 6, body, 0)


def to_chunks(lines, k, chunks):
    def body(h, carry):
        for tau in range(2):
            for top in range(2):
                row = k * 12 + tau * 6 + h
                base = pl.multiple_of(h * 64, 64)
                lanes = slice((top * 2 + tau) * 128, (top * 2 + tau + 1) * 128)
                got = [lines[pl.ds(base + x8 * 8, 8), lanes] for x8 in range(8)]
                for p, piece in enumerate(swap_lanes(got)):
                    chunks[pl.ds((top * 8 + p) * 8 * ROWS + row, 8, stride=ROWS), :] = piece
        return carry

    lax.fori_loop(0, 6, body, 0)


def pack_rows(field, packed):
    def body(i, carry):
        tau, h = i // 6, i % 6
        v = field[pl.ds(pl.multiple_of(tau * 16, 16), 16), pl.ds(pl.multiple_of(h * 8, 8), 8), :]
        high, low = split(v.reshape(128, 384))
        rows = pl.ds(pl.multiple_of(i * 128, 128), 128)
        packed[rows, 0:384] = high
        packed[rows, 384:768] = low
        packed[rows, 768:1152] = high
        return carry

    lax.fori_loop(0, 12, body, 0)


def forward_y(packed, left, chunks):
    def body(i, carry):
        out = dot(left[...], packed[pl.ds(pl.multiple_of(i * 256, 256), 256), :], 1, 1)
        for k in range(3):
            for j in range(2):
                chunks[pl.ds(k * 12 + i * 2 + j, 128, stride=ROWS), :] = out[
                    k * 128 : (k + 1) * 128, j * 128 : (j + 1) * 128
                ]
        return carry

    lax.fori_loop(0, 6, body, 0)


def tripled(ref, values):
    high, low = split(values)
    width = values.shape[1]
    ref[:, 0:width] = high
    ref[:, width : 2 * width] = high
    ref[:, 2 * width : 3 * width] = low


def stacked(values):
    high, low = split(values)
    return jnp.concatenate([high, low, high], axis=0)


def forward_tx(lines, time_high, time_low, left_x):
    high, low = split(lines[...])
    mid = dot(high, time_high[...]) + dot(high, time_low[...]) + dot(low, time_high[...])
    return dot(left_x[...], stacked(mid))


def send_all(where, copy_to):
    def body(i, carry):
        copy_to(*partner(i, where)).start()
        return carry

    lax.fori_loop(1, 128, body, 0)


def stencil(ext, reac, ycoef, xcoef, tbands, first_t, tcoef, mass, stiff, mixed, rest, image):
    def time_weight(matrix, off, t):
        size = abs(off)
        if off <= 0:
            value = tbands[matrix, size, jnp.maximum(t - size, 0)]
            return jnp.where(t >= size, value, 0.0)
        return jnp.where(t + size < 512, tbands[matrix, size, t], 0.0)

    def along_y(t, carry):
        for part in range(2):
            rows = slice(part * 32, part * 32 + 32)
            v = ext[t, rows, :]
            m = ycoef[3:4, :] * v
            s = ycoef[10:11, :] * v
            for off in (-3, -2, -1, 1, 2, 3):
                moved = pltpu.roll(v, (-off) % 384, 1)
                m = m + ycoef[3 + off : 4 + off, :] * moved
                s = s + ycoef[10 + off : 11 + off, :] * moved
            for c in range(3):
                mass[t, c, rows, :] = m[:, c * 128 : (c + 1) * 128]
                stiff[t, c, rows, :] = s[:, c * 128 : (c + 1) * 128]
        return carry

    lax.fori_loop(0, 38, along_y, 0)

    for i in range(6):
        first = i * 8
        ms = [xcoef[j, first : first + 8, :] for j in range(7)]
        ks = [xcoef[7 + j, first : first + 8, :] for j in range(7)]

        def along_x(t, carry):
            for c in range(3):
                m = [mass[t, c, 5 + j + first : 13 + j + first, :] for j in range(7)]
                s = [stiff[t, c, 5 + j + first : 13 + j + first, :] for j in range(7)]
                a = ms[0] * m[0]
                b = ks[0] * m[0] + ms[0] * s[0]
                for j in range(1, 7):
                    a = a + ms[j] * m[j]
                    b = b + (ks[j] * m[j] + ms[j] * s[j])
                mixed[t, c, first : first + 8, :] = a
                rest[t, c, first : first + 8, :] = b
            return carry

        lax.fori_loop(0, 38, along_x, 0)

    def weights(t, carry):
        for j in range(7):
            tcoef[t * 14 + j] = time_weight(0, j - 3, first_t + t)
            tcoef[t * 14 + 7 + j] = time_weight(1, j - 3, first_t + t)
        return carry

    lax.fori_loop(0, 32, weights, 0)

    def along_t(pair, total):
        t = pair * 2
        kt = [[tcoef[(t + n) * 14 + j] for j in range(7)] for n in range(2)]
        mt = [[tcoef[(t + n) * 14 + 7 + j] for j in range(7)] for n in range(2)]
        for c in range(3):
            lanes = slice(c * 128, c * 128 + 128)
            for i in range(6):
                rows = slice(i * 8, i * 8 + 8)
                own = [ext[t + 3 + n, 8 + i * 8 : 16 + i * 8, lanes] for n in range(2)]
                value = [reac[t + n, rows, lanes] * own[n] for n in range(2)]
                for j in range(8):
                    a = mixed[t + j, c, rows, :]
                    b = rest[t + j, c, rows, :]
                    for n in range(2):
                        if 0 <= j - n < 7:
                            value[n] = value[n] + (kt[n][j - n] * a + mt[n][j - n] * b)
                for n in range(2):
                    image[t + n, rows, lanes] = value[n]
                    total = total + own[n] * value[n]
        return total

    return lax.fori_loop(0, 16, along_t, jnp.zeros((8, 128), F32))


def whole(x):
    return jnp.sum(jnp.sum(x, axis=1, keepdims=True), axis=0, keepdims=True)


def band_lines(table):
    lane = lax.broadcasted_iota(jnp.int32, (1, 384), 1)
    lines = []
    for off in range(-3, 4):
        size = abs(off)
        line = table[size : size + 1, :]
        if off < 0:
            line = jnp.where(lane >= size, pltpu.roll(line, size, 1), 0.0)
        elif off > 0:
            line = jnp.where(lane < 384 - size, line, 0.0)
        lines.append(line)
    return lines


def main_kernel(
    r_h, d_h, reac_h, s_h, t_h, sb_h, te_h, se_h, tbands, seig,
    img_h, back_h, scal_o,
    rv, ext, reac, image, s_v, s3, t4, sb_v, te_v, se_v, base_v, yc_v, xt_v, xc_v, sp_v,
    left_y, left_x, left_xi, time_high, time_low, packed,
    send1, send2, recv1, recv2, lines, hat_r,
    mass, stiff, mixed, rest, red1s, red1, red2s, red2,
    tcoef, local, halo_s, halo_r, out_sem, send_sem, recv_sem,
):
    where = position()
    tm = lax.axis_index("tm")
    sp = lax.axis_index("space")
    me = tm * 8 + sp
    pairs = [(d_h, ext.at[3:35, 8:56]), (s_h, s_v), (r_h, rv), (sb_h, sb_v), (reac_h, reac), (te_h, te_v), (se_h, se_v)]
    pairs += [(s_h.at[:, c * 128 : c * 128 + 128], s3.at[c]) for c in range(3)]
    pairs += [(t_h.at[:, c * 128 : c * 128 + 128], t4.at[c]) for c in range(4)]
    loads = [pltpu.make_async_copy(src, dst, local.at[n]) for n, (src, dst) in enumerate(pairs)]
    for load in loads:
        load.start()

    barrier = pltpu.get_barrier_semaphore()

    def greet(i, carry):
        pl.semaphore_signal(barrier, inc=1, device_id=partner(i, where), device_id_type=MESH)
        return carry

    lax.fori_loop(1, 128, greet, 0)
    loads[1].wait()
    tripled(left_y, s_v[...].T)
    loads[2].wait()
    pack_rows(rv, packed)
    forward_y(packed, left_y, send1)
    loads[0].wait()
    pl.semaphore_wait(barrier, 127)

    halos = []
    for dt, src_t, dst_t in ((-1, slice(3, 6), slice(35, 38)), (0, slice(3, 35), slice(3, 35)), (1, slice(32, 35), slice(0, 3))):
        for dx, src_x, dst_x in ((-1, slice(8, 11), slice(56, 59)), (0, slice(8, 56), slice(8, 56)), (1, slice(53, 56), slice(5, 8))):
            if dt or dx:
                n = len(halos)
                halos.append(
                    pltpu.make_async_remote_copy(
                        src_ref=ext.at[src_t, src_x],
                        dst_ref=ext.at[dst_t, dst_x],
                        send_sem=halo_s.at[n],
                        recv_sem=halo_r.at[n],
                        device_id=((tm + 16 + dt) % 16, (sp + 8 + dx) % 8),
                        device_id_type=MESH,
                    )
                )
    for halo in halos:
        halo.start()

    def piece(ref, d, k):
        return ref.at[pl.ds(d * ROWS + k * 12, 12)]

    def exchange(n, src, dst, k):
        def copy_to(t, s):
            return pltpu.make_async_remote_copy(
                src_ref=piece(src, t * 8 + s, k),
                dst_ref=piece(dst, me, k),
                send_sem=send_sem.at[n * 3 + k],
                recv_sem=recv_sem.at[n * 3 + k],
                device_id=(t, s),
                device_id_type=MESH,
            )

        send_all(where, copy_to)

    def finish(n, src, dst, rows):
        return pltpu.make_async_remote_copy(
            src_ref=src.at[pl.ds(0, 127 * rows)],
            dst_ref=dst.at[pl.ds(0, 127 * rows)],
            send_sem=send_sem.at[n],
            recv_sem=recv_sem.at[n],
            device_id=(tm, sp),
            device_id_type=MESH,
        )

    def own_chunk(src, dst):
        dst[pl.ds(me * ROWS, ROWS), :] = src[pl.ds(me * ROWS, ROWS), :]

    for k in range(3):
        exchange(0, send1, recv1, k)
    own_chunk(send1, recv1)

    loads[3].wait()
    table = jnp.concatenate(band_lines(sb_v[1]) + band_lines(sb_v[0]) + [jnp.zeros((2, 384), F32)], axis=0)
    yc_v[...] = table
    xt_v[...] = table.T
    near = xt_v[pl.ds(pl.multiple_of(sp * 48, 16), 48), :]
    for j in range(14):
        xc_v[j] = jnp.broadcast_to(near[:, j : j + 1], (48, 128))
    for load in loads[4:]:
        load.wait()
    for halo in halos:
        halo.wait()
    curve = stencil(ext, reac, yc_v, xc_v, tbands, tm * 32, tcoef, mass, stiff, mixed, rest, image)
    store_image = pltpu.make_async_copy(image, img_h, out_sem.at[0])
    store_image.start()
    pack_rows(image, packed)

    forward_y(packed, left_y, send2)
    exchange(1, send2, recv2, 0)
    exchange(1, send2, recv2, 1)
    own_chunk(send2, recv2)

    for h in range(48):
        for c in range(3):
            sp_v[h * 8 : h * 8 + 8, c * 128 : c * 128 + 128] = s3[c, pl.ds(h, 8, stride=48), :]
    tripled(left_x, sp_v[...].T)
    tripled(left_xi, sp_v[...])

    def time_rows(i, carry):
        start = (i // 16) * 256 + (i // 8) % 2 * 16 + i % 8 * 2
        rows = pl.ds(pl.multiple_of(i * 16, 16), 16)
        for c in range(4):
            got = jnp.concatenate([t4[c, pl.ds(start + j, 8, stride=32), :] for j in range(2)], axis=0)
            high, low = split(got)
            time_high[rows, c * 128 : c * 128 + 128] = high
            time_low[rows, c * 128 : c * 128 + 128] = low
        return carry

    lax.fori_loop(0, 32, time_rows, 0)
    column = jnp.broadcast_to(se_v[...], (8, 384)).T
    base_v[...] = column[:, 0:1] + te_v[...]

    def eigen(k):
        return base_v[...] + seig[k * 128 + me]

    def old_part(k, total):
        finish(k, send1, recv1, 12).wait()
        to_lines(recv1, k, lines)
        v = forward_tx(lines, time_high, time_low, left_x)
        hat_r[pl.ds(pl.multiple_of(k * 384, 384), 384), :] = v
        return total + jnp.sum((v * (v / eigen(k))).reshape(48, 8, 512), axis=0)

    old = lax.fori_loop(0, 3, old_part, jnp.zeros((8, 512), F32))
    old = old[:, 0:128] + old[:, 128:256] + old[:, 256:384] + old[:, 384:512]

    def share(n, mine, every, rows):
        def copy_to(t, s):
            return pltpu.make_async_remote_copy(
                src_ref=mine,
                dst_ref=every.at[pl.ds(me * rows, rows)],
                send_sem=send_sem.at[n],
                recv_sem=recv_sem.at[n],
                device_id=(t, s),
                device_id_type=MESH,
            )

        send_all(where, copy_to)
        every[pl.ds(me * rows, rows), :] = mine[...]

    red1s[0:1, :] = jnp.sum(old, axis=0, keepdims=True)
    red1s[1:2, :] = jnp.sum(curve, axis=0, keepdims=True)
    share(9, red1s, red1, 2)
    exchange(1, send2, recv2, 2)

    finish(9, red1, red1, 2).wait()
    every = red1[...]
    even = lax.broadcasted_iota(jnp.int32, (256, 128), 0) % 2 == 0
    norm_old = whole(jnp.where(even, every, 0.0))
    step = norm_old / whole(jnp.where(even, 0.0, every))

    def inverse_part(k, total):
        finish(3 + k, send2, recv2, 12).wait()
        to_lines(recv2, k, lines)
        rows = pl.ds(pl.multiple_of(k * 384, 384), 384)
        v = hat_r[rows, :] - step * forward_tx(lines, time_high, time_low, left_x)
        g = v / eigen(k)
        high, low = split(dot(left_xi[...], stacked(g)))
        lines[...] = (
            dot(high, time_high[...], 1, 1)
            + dot(high, time_low[...], 1, 1)
            + dot(low, time_high[...], 1, 1)
        )
        to_chunks(lines, k, send1)
        exchange(2, send1, back_h, k)
        return total + jnp.sum((v * g).reshape(48, 8, 512), axis=0)

    new = lax.fori_loop(0, 3, inverse_part, jnp.zeros((8, 512), F32))
    own = pltpu.make_async_copy(
        send1.at[pl.ds(me * ROWS, ROWS)], back_h.at[pl.ds(me * ROWS, ROWS)], out_sem.at[1]
    )
    own.start()

    new = new[:, 0:128] + new[:, 128:256] + new[:, 256:384] + new[:, 384:512]
    red2s[...] = jnp.sum(new, axis=0, keepdims=True)
    share(10, red2s, red2, 1)
    finish(10, red2, red2, 1).wait()
    norm_new = whole(red2[...])
    row = lax.broadcasted_iota(jnp.int32, (8, 128), 0)
    scal_o[...] = jnp.where(row == 0, step, norm_new / norm_old)

    store_image.wait()
    own.wait()
    for k in range(3):
        finish(6 + k, send1, back_h, 12).wait()


def last_kernel(
    back_h, s_h, d_h, sol_h, r_h, img_h, scal,
    new_sol, new_res, new_dir,
    back, s_v, left, d_v, sol_v, r_v, img_v, ns_v, nr_v, nd_v, in_sem, out_sem,
):
    start = [pltpu.make_async_copy(s_h, s_v, in_sem.at[0]), pltpu.make_async_copy(back_h, back, in_sem.at[1])]
    halves = []
    for half in range(2):
        t = slice(half * 16, half * 16 + 16)
        halves.append(
            [
                pltpu.make_async_copy(src.at[t], dst.at[t], in_sem.at[2 + half * 4 + n])
                for n, (src, dst) in enumerate(((d_h, d_v), (sol_h, sol_v), (r_h, r_v), (img_h, img_v)))
            ]
        )
    for copy in start + halves[0] + halves[1]:
        copy.start()
    start[0].wait()
    tripled(left, s_v[...])
    start[1].wait()
    step = scal[0:1, 0:1]
    ratio = scal[1:2, 0:1]
    stores = []
    for tau in range(2):
        t = slice(tau * 16, tau * 16 + 16)
        for copy in halves[tau]:
            copy.wait()

        def body(i, carry):
            h = i * 2
            parts = []
            for j in range(2):
                parts.append(
                    jnp.concatenate(
                        [back[pl.ds(k * 12 + tau * 6 + h + j, 128, stride=ROWS), :] for k in range(3)], axis=0
                    )
                )
            out = dot(left[...], stacked(jnp.concatenate(parts, axis=1))).T
            for j in range(2):
                x = pl.ds(pl.multiple_of((h + j) * 8, 8), 8)
                d = d_v[t, x, :]
                nd_v[t, x, :] = out[j * 128 : (j + 1) * 128, :].reshape(16, 8, 384) + ratio.reshape(1, 1, 1) * d
                ns_v[t, x, :] = sol_v[t, x, :] + step.reshape(1, 1, 1) * d
                nr_v[t, x, :] = r_v[t, x, :] - step.reshape(1, 1, 1) * img_v[t, x, :]
            return carry

        lax.fori_loop(0, 3, body, 0)
        for n, (src, dst) in enumerate(((ns_v, new_sol), (nr_v, new_res), (nd_v, new_dir))):
            stores.append(pltpu.make_async_copy(src.at[t], dst.at[t], out_sem.at[tau * 3 + n]))
            stores[-1].start()
    for store in stores:
        store.wait()


VMEM = pl.BlockSpec(memory_space=pltpu.VMEM)
HBM = pl.BlockSpec(memory_space=pltpu.HBM)
SMEM = pl.BlockSpec(memory_space=pltpu.SMEM)


def per_device(solution, residual, direction, reaction, time_bands, space_bands, time_basis, space_basis, time_eigen, space_eigen):
    block = (32, 48, 384)
    chunks = (128 * ROWS, 128)
    v = pltpu.VMEM
    dma = pltpu.SemaphoreType.DMA
    image, back, scal = pl.pallas_call(
        main_kernel,
        out_shape=(
            jax.ShapeDtypeStruct(block, F32),
            jax.ShapeDtypeStruct(chunks, F32),
            jax.ShapeDtypeStruct((8, 128), F32),
        ),
        in_specs=[HBM] * 8 + [SMEM] * 2,
        out_specs=(HBM, HBM, VMEM),
        scratch_shapes=[
            v(block, F32), v((38, 64, 384), F32), v(block, F32), v(block, F32),
            v((384, 384), F32), v((3, 384, 128), F32), v((4, 512, 128), F32), v((2, 4, 384), F32),
            v((1, 512), F32), v((1, 384), F32), v((384, 512), F32),
            v((16, 384), F32), v((384, 16), F32), v((14, 48, 128), F32), v((384, 384), F32),
            v((384, 1152), BF16), v((384, 1152), BF16), v((384, 1152), BF16),
            v((512, 512), BF16), v((512, 512), BF16), v((1536, 1152), BF16),
            v(chunks, F32), v(chunks, F32), v(chunks, F32), v(chunks, F32),
            v((384, 512), F32), v((1152, 512), F32),
            v((38, 3, 64, 128), F32), v((38, 3, 64, 128), F32),
            v((38, 3, 48, 128), F32), v((38, 3, 48, 128), F32),
            v((2, 128), F32), v((256, 128), F32), v((1, 128), F32), v((128, 128), F32),
            pltpu.SMEM((448,), F32), dma((14,)), dma((8,)), dma((8,)), dma((2,)), dma((11,)), dma((11,)),
        ],
        compiler_params=pltpu.CompilerParams(
            collective_id=0, has_side_effects=True, vmem_limit_bytes=62 * 2**20
        ),
    )(
        residual, direction, reaction, space_basis, time_basis, space_bands,
        time_eigen.reshape(1, -1), space_eigen.reshape(1, -1), time_bands, space_eigen,
    )
    return pl.pallas_call(
        last_kernel,
        out_shape=(jax.ShapeDtypeStruct(block, F32),) * 3,
        in_specs=[HBM] * 6 + [VMEM],
        out_specs=(HBM,) * 3,
        scratch_shapes=[
            v(chunks, F32), v((384, 384), F32), v((384, 1152), BF16),
            *[v(block, F32) for _ in range(7)],
            dma((10,)), dma((6,)),
        ],
        compiler_params=pltpu.CompilerParams(vmem_limit_bytes=62 * 2**20),
    )(back, space_basis, direction, solution, residual, image, scal)


def solution(mesh):
    field = P("tm", "space", None)
    return jax.shard_map(
        per_device,
        mesh=mesh,
        in_specs=(field,) * 4 + (P(),) * 6,
        out_specs=(field,) * 3,
        check_vma=False,
    )
```

```python
import jax
import jax.numpy as jnp
from jax import lax
from jax.experimental import pallas as pl
from jax.experimental.pallas import tpu as pltpu
from jax.sharding import PartitionSpec as P

F32 = jnp.float32
BF16 = jnp.bfloat16
MESH = pl.DeviceIdType.MESH
ROWS = 36


def split(x):
    high = x.astype(BF16)
    return high, (x - high.astype(F32)).astype(BF16)


def dot(a, b, ca=1, cb=0):
    return lax.dot_general(a, b, (((ca,), (cb,)), ((), ())), preferred_element_type=F32)


def position():
    tm = lax.axis_index("tm")
    sp = lax.axis_index("space")
    return tm // 4, (tm // 2) % 2 * 2 + sp // 4, sp % 4, tm % 2


def device(z, x, y, c):
    return z * 4 + (x // 2) * 2 + c, (x % 2) * 4 + y


def wrapped(v):
    return jnp.where(v >= 4, v - 4, v)


def each_partner(where, act):
    z, x, y, c = where
    tops = [wrapped(z + a) * 4 for a in range(4)]
    cores = [c, 1 - c]

    def outer(b, carry):
        def inner(e, carry):
            xb = wrapped(x + b)
            yb = wrapped(wrapped(y + b) + e)
            for a in range(4):
                xa = wrapped(xb + a)
                high = jnp.where(xa >= 2, 2, 0)
                s = (xa - high) * 4 + wrapped(yb + a)
                for d in range(2):
                    t = tops[a] + high + cores[(a + d) % 2]
                    if a == 0 and d == 0:
                        pl.when(b + e > 0)(lambda: act(t, s))
                    else:
                        act(t, s)
            return carry

        return lax.fori_loop(0, 4, inner, carry)

    lax.fori_loop(0, 4, outer, 0)


def swap_lanes(pieces):
    lane = lax.broadcasted_iota(jnp.int32, (8, 128), 1)
    for bit in (1, 2, 4):
        low = (lane & bit) == 0
        moved = list(pieces)
        for p in range(8):
            if p & bit == 0:
                a, b = pieces[p], pieces[p | bit]
                moved[p] = jnp.where(low, a, pltpu.roll(b, bit, 1))
                moved[p | bit] = jnp.where(low, pltpu.roll(a, 128 - bit, 1), b)
        pieces = moved
    return pieces


def to_lines(chunks, k, lines):
    def body(h, carry):
        for tau in range(2):
            for top in range(2):
                row = k * 12 + tau * 6 + h
                got = [
                    chunks[pl.ds((top * 8 + p) * 8 * ROWS + row, 8, stride=ROWS), :]
                    for p in range(8)
                ]
                base = pl.multiple_of(h * 64, 64)
                lanes = slice((top * 2 + tau) * 128, (top * 2 + tau + 1) * 128)
                for x8, piece in enumerate(swap_lanes(got)):
                    lines[pl.ds(base + x8 * 8, 8), lanes] = piece
        return carry

    lax.fori_loop(0, 6, body, 0)


def to_chunks(lines, k, chunks):
    def body(h, carry):
        for tau in range(2):
            for top in range(2):
                row = k * 12 + tau * 6 + h
                base = pl.multiple_of(h * 64, 64)
                lanes = slice((top * 2 + tau) * 128, (top * 2 + tau + 1) * 128)
                got = [lines[pl.ds(base + x8 * 8, 8), lanes] for x8 in range(8)]
                for p, piece in enumerate(swap_lanes(got)):
                    chunks[pl.ds((top * 8 + p) * 8 * ROWS + row, 8, stride=ROWS), :] = piece
        return carry

    lax.fori_loop(0, 6, body, 0)


def pack_rows(field, packed):
    def body(i, carry):
        tau, h = i // 6, i % 6
        v = field[pl.ds(pl.multiple_of(tau * 16, 16), 16), pl.ds(pl.multiple_of(h * 8, 8), 8), :]
        high, low = split(v.reshape(128, 384))
        rows = pl.ds(pl.multiple_of(i * 128, 128), 128)
        packed[rows, 0:384] = high
        packed[rows, 384:768] = low
        packed[rows, 768:1152] = high
        return carry

    lax.fori_loop(0, 12, body, 0)


def forward_y(packed, left, chunks):
    def body(i, carry):
        out = dot(left[...], packed[pl.ds(pl.multiple_of(i * 256, 256), 256), :], 1, 1)
        for k in range(3):
            for j in range(2):
                chunks[pl.ds(k * 12 + i * 2 + j, 128, stride=ROWS), :] = out[
                    k * 128 : (k + 1) * 128, j * 128 : (j + 1) * 128
                ]
        return carry

    lax.fori_loop(0, 6, body, 0)


def tripled(ref, values):
    high, low = split(values)
    width = values.shape[1]
    ref[:, 0:width] = high
    ref[:, width : 2 * width] = high
    ref[:, 2 * width : 3 * width] = low


def stacked(values):
    high, low = split(values)
    return jnp.concatenate([high, low, high], axis=0)


def forward_tx(lines, time_high, time_low, left_x):
    high, low = split(lines[...])
    mid = dot(high, time_high[...]) + dot(high, time_low[...]) + dot(low, time_high[...])
    return dot(left_x[...], stacked(mid))


def send_all(where, copy_to):
    each_partner(where, lambda t, s: copy_to(t, s).start())


def stencil(ext, reac, ycoef, xcoef, tbands, first_t, tcoef, mass, stiff, mixed, rest, image):
    def time_weight(matrix, off, t):
        size = abs(off)
        if off <= 0:
            value = tbands[matrix, size, jnp.maximum(t - size, 0)]
            return jnp.where(t >= size, value, 0.0)
        return jnp.where(t + size < 512, tbands[matrix, size, t], 0.0)

    def along_y(t, carry):
        for part in range(2):
            rows = slice(part * 32, part * 32 + 32)
            v = ext[t, rows, :]
            m = ycoef[3:4, :] * v
            s = ycoef[10:11, :] * v
            for off in (-3, -2, -1, 1, 2, 3):
                moved = pltpu.roll(v, (-off) % 384, 1)
                m = m + ycoef[3 + off : 4 + off, :] * moved
                s = s + ycoef[10 + off : 11 + off, :] * moved
            for c in range(3):
                mass[t, c, rows, :] = m[:, c * 128 : (c + 1) * 128]
                stiff[t, c, rows, :] = s[:, c * 128 : (c + 1) * 128]
        return carry

    lax.fori_loop(0, 38, along_y, 0)

    for i in range(6):
        first = i * 8
        ms = [xcoef[j, first : first + 8, :] for j in range(7)]
        ks = [xcoef[7 + j, first : first + 8, :] for j in range(7)]

        def along_x(t, carry):
            for c in range(3):
                m = [mass[t, c, 5 + j + first : 13 + j + first, :] for j in range(7)]
                s = [stiff[t, c, 5 + j + first : 13 + j + first, :] for j in range(7)]
                a = ms[0] * m[0]
                b = ks[0] * m[0] + ms[0] * s[0]
                for j in range(1, 7):
                    a = a + ms[j] * m[j]
                    b = b + (ks[j] * m[j] + ms[j] * s[j])
                mixed[t, c, first : first + 8, :] = a
                rest[t, c, first : first + 8, :] = b
            return carry

        lax.fori_loop(0, 38, along_x, 0)

    def weights(t, carry):
        for j in range(7):
            tcoef[t * 14 + j] = time_weight(0, j - 3, first_t + t)
            tcoef[t * 14 + 7 + j] = time_weight(1, j - 3, first_t + t)
        return carry

    lax.fori_loop(0, 32, weights, 0)

    def along_t(pair, total):
        t = pair * 2
        kt = [[tcoef[(t + n) * 14 + j] for j in range(7)] for n in range(2)]
        mt = [[tcoef[(t + n) * 14 + 7 + j] for j in range(7)] for n in range(2)]
        for c in range(3):
            lanes = slice(c * 128, c * 128 + 128)
            for i in range(6):
                rows = slice(i * 8, i * 8 + 8)
                own = [ext[t + 3 + n, 8 + i * 8 : 16 + i * 8, lanes] for n in range(2)]
                value = [reac[t + n, rows, lanes] * own[n] for n in range(2)]
                for j in range(8):
                    a = mixed[t + j, c, rows, :]
                    b = rest[t + j, c, rows, :]
                    for n in range(2):
                        if 0 <= j - n < 7:
                            value[n] = value[n] + (kt[n][j - n] * a + mt[n][j - n] * b)
                for n in range(2):
                    image[t + n, rows, lanes] = value[n]
                    total = total + own[n] * value[n]
        return total

    return lax.fori_loop(0, 16, along_t, jnp.zeros((8, 128), F32))


def whole(x):
    return jnp.sum(jnp.sum(x, axis=1, keepdims=True), axis=0, keepdims=True)


def band_lines(table):
    lane = lax.broadcasted_iota(jnp.int32, (1, 384), 1)
    lines = []
    for off in range(-3, 4):
        size = abs(off)
        line = table[size : size + 1, :]
        if off < 0:
            line = jnp.where(lane >= size, pltpu.roll(line, size, 1), 0.0)
        elif off > 0:
            line = jnp.where(lane < 384 - size, line, 0.0)
        lines.append(line)
    return lines


def main_kernel(
    r_h, d_h, reac_h, s_h, t_h, sb_h, te_h, se_h, tbands, seig,
    img_h, back_h, scal_o,
    rv, ext, reac, image, s_v, s3, t4, sb_v, te_v, se_v, base_v, yc_v, xt_v, xc_v, sp_v,
    left_y, left_x, left_xi, time_high, time_low, packed,
    send1, send2, recv1, recv2, lines, hat_r,
    mass, stiff, mixed, rest, red1s, red1, red2s, red2,
    tcoef, local, halo_s, halo_r, out_sem, send_sem, recv_sem,
):
    where = position()
    tm = lax.axis_index("tm")
    sp = lax.axis_index("space")
    me = tm * 8 + sp
    pairs = [(d_h, ext.at[3:35, 8:56]), (s_h, s_v), (r_h, rv), (sb_h, sb_v), (reac_h, reac), (te_h, te_v), (se_h, se_v)]
    pairs += [(s_h.at[:, c * 128 : c * 128 + 128], s3.at[c]) for c in range(3)]
    pairs += [(t_h.at[:, c * 128 : c * 128 + 128], t4.at[c]) for c in range(4)]
    loads = [pltpu.make_async_copy(src, dst, local.at[n]) for n, (src, dst) in enumerate(pairs)]
    for load in loads:
        load.start()

    barrier = pltpu.get_barrier_semaphore()

    each_partner(
        where,
        lambda t, s: pl.semaphore_signal(barrier, inc=1, device_id=(t, s), device_id_type=MESH),
    )
    loads[1].wait()
    tripled(left_y, s_v[...].T)
    loads[2].wait()
    pack_rows(rv, packed)
    forward_y(packed, left_y, send1)
    loads[0].wait()
    pl.semaphore_wait(barrier, 127)

    halos = []
    for dt, src_t, dst_t in ((-1, slice(3, 6), slice(35, 38)), (0, slice(3, 35), slice(3, 35)), (1, slice(32, 35), slice(0, 3))):
        for dx, src_x, dst_x in ((-1, slice(8, 11), slice(56, 59)), (0, slice(8, 56), slice(8, 56)), (1, slice(53, 56), slice(5, 8))):
            if dt or dx:
                n = len(halos)
                halos.append(
                    pltpu.make_async_remote_copy(
                        src_ref=ext.at[src_t, src_x],
                        dst_ref=ext.at[dst_t, dst_x],
                        send_sem=halo_s.at[n],
                        recv_sem=halo_r.at[n],
                        device_id=((tm + 16 + dt) % 16, (sp + 8 + dx) % 8),
                        device_id_type=MESH,
                    )
                )
    for halo in halos:
        halo.start()

    def exchange(n, src, dst, start, rows):
        def copy_to(t, s):
            return pltpu.make_async_remote_copy(
                src_ref=src.at[pl.ds((t * 8 + s) * ROWS + start, rows)],
                dst_ref=dst.at[pl.ds(me * ROWS + start, rows)],
                send_sem=send_sem.at[n],
                recv_sem=recv_sem.at[n],
                device_id=(t, s),
                device_id_type=MESH,
            )

        send_all(where, copy_to)

    def finish(n, src, dst, rows):
        return pltpu.make_async_remote_copy(
            src_ref=src.at[pl.ds(0, 127 * rows)],
            dst_ref=dst.at[pl.ds(0, 127 * rows)],
            send_sem=send_sem.at[n],
            recv_sem=recv_sem.at[n],
            device_id=(tm, sp),
            device_id_type=MESH,
        )

    def own_chunk(src, dst):
        dst[pl.ds(me * ROWS, ROWS), :] = src[pl.ds(me * ROWS, ROWS), :]

    exchange(0, send1, recv1, 0, ROWS)
    own_chunk(send1, recv1)

    loads[3].wait()
    table = jnp.concatenate(band_lines(sb_v[1]) + band_lines(sb_v[0]) + [jnp.zeros((2, 384), F32)], axis=0)
    yc_v[...] = table
    xt_v[...] = table.T
    near = xt_v[pl.ds(pl.multiple_of(sp * 48, 16), 48), :]
    for j in range(14):
        xc_v[j] = jnp.broadcast_to(near[:, j : j + 1], (48, 128))
    for load in loads[4:]:
        load.wait()
    for halo in halos:
        halo.wait()
    curve = stencil(ext, reac, yc_v, xc_v, tbands, tm * 32, tcoef, mass, stiff, mixed, rest, image)
    store_image = pltpu.make_async_copy(image, img_h, out_sem.at[0])
    store_image.start()
    pack_rows(image, packed)

    forward_y(packed, left_y, send2)
    exchange(1, send2, recv2, 0, 24)
    own_chunk(send2, recv2)

    for h in range(48):
        for c in range(3):
            sp_v[h * 8 : h * 8 + 8, c * 128 : c * 128 + 128] = s3[c, pl.ds(h, 8, stride=48), :]
    tripled(left_x, sp_v[...].T)
    tripled(left_xi, sp_v[...])

    def time_rows(i, carry):
        start = (i // 16) * 256 + (i // 8) % 2 * 16 + i % 8 * 2
        rows = pl.ds(pl.multiple_of(i * 16, 16), 16)
        for c in range(4):
            got = jnp.concatenate([t4[c, pl.ds(start + j, 8, stride=32), :] for j in range(2)], axis=0)
            high, low = split(got)
            time_high[rows, c * 128 : c * 128 + 128] = high
            time_low[rows, c * 128 : c * 128 + 128] = low
        return carry

    lax.fori_loop(0, 32, time_rows, 0)
    column = jnp.broadcast_to(se_v[...], (8, 384)).T
    base_v[...] = column[:, 0:1] + te_v[...]

    def eigen(k):
        return base_v[...] + seig[k * 128 + me]

    def old_part(k, total):
        to_lines(recv1, k, lines)
        v = forward_tx(lines, time_high, time_low, left_x)
        hat_r[pl.ds(pl.multiple_of(k * 384, 384), 384), :] = v
        return total + jnp.sum((v * (v / eigen(k))).reshape(48, 8, 512), axis=0)

    finish(0, send1, recv1, ROWS).wait()
    old = lax.fori_loop(0, 3, old_part, jnp.zeros((8, 512), F32))
    old = old[:, 0:128] + old[:, 128:256] + old[:, 256:384] + old[:, 384:512]

    def share(n, mine, every, rows):
        def copy_to(t, s):
            return pltpu.make_async_remote_copy(
                src_ref=mine,
                dst_ref=every.at[pl.ds(me * rows, rows)],
                send_sem=send_sem.at[n],
                recv_sem=recv_sem.at[n],
                device_id=(t, s),
                device_id_type=MESH,
            )

        send_all(where, copy_to)
        every[pl.ds(me * rows, rows), :] = mine[...]

    red1s[0:1, :] = jnp.sum(old, axis=0, keepdims=True)
    red1s[1:2, :] = jnp.sum(curve, axis=0, keepdims=True)
    share(6, red1s, red1, 2)
    exchange(2, send2, recv2, 24, 12)

    finish(1, send2, recv2, 24).wait()
    finish(6, red1, red1, 2).wait()
    every = red1[...]
    even = lax.broadcasted_iota(jnp.int32, (256, 128), 0) % 2 == 0
    norm_old = whole(jnp.where(even, every, 0.0))
    step = norm_old / whole(jnp.where(even, 0.0, every))

    def inverse_part(k, total):
        @pl.when(k == 2)
        def _():
            finish(2, send2, recv2, 12).wait()

        to_lines(recv2, k, lines)
        rows = pl.ds(pl.multiple_of(k * 384, 384), 384)
        v = hat_r[rows, :] - step * forward_tx(lines, time_high, time_low, left_x)
        g = v / eigen(k)
        high, low = split(dot(left_xi[...], stacked(g)))
        lines[...] = (
            dot(high, time_high[...], 1, 1)
            + dot(high, time_low[...], 1, 1)
            + dot(low, time_high[...], 1, 1)
        )
        to_chunks(lines, k, send1)
        exchange(3 + k, send1, back_h, k * 12, 12)
        return total + jnp.sum((v * g).reshape(48, 8, 512), axis=0)

    new = lax.fori_loop(0, 3, inverse_part, jnp.zeros((8, 512), F32))
    own = pltpu.make_async_copy(
        send1.at[pl.ds(me * ROWS, ROWS)], back_h.at[pl.ds(me * ROWS, ROWS)], out_sem.at[1]
    )
    own.start()

    new = new[:, 0:128] + new[:, 128:256] + new[:, 256:384] + new[:, 384:512]
    red2s[...] = jnp.sum(new, axis=0, keepdims=True)
    share(7, red2s, red2, 1)
    finish(7, red2, red2, 1).wait()
    norm_new = whole(red2[...])
    row = lax.broadcasted_iota(jnp.int32, (8, 128), 0)
    scal_o[...] = jnp.where(row == 0, step, norm_new / norm_old)

    store_image.wait()
    own.wait()
    for k in range(3):
        finish(3 + k, send1, back_h, 12).wait()


def last_kernel(
    back_h, s_h, d_h, sol_h, r_h, img_h, scal,
    new_sol, new_res, new_dir,
    back, s_v, left, d_v, sol_v, r_v, img_v, ns_v, nr_v, nd_v, in_sem, out_sem,
):
    start = [pltpu.make_async_copy(s_h, s_v, in_sem.at[0]), pltpu.make_async_copy(back_h, back, in_sem.at[1])]
    halves = []
    for half in range(2):
        t = slice(half * 16, half * 16 + 16)
        halves.append(
            [
                pltpu.make_async_copy(src.at[t], dst.at[t], in_sem.at[2 + half * 4 + n])
                for n, (src, dst) in enumerate(((d_h, d_v), (sol_h, sol_v), (r_h, r_v), (img_h, img_v)))
            ]
        )
    for copy in start + halves[0] + halves[1]:
        copy.start()
    start[0].wait()
    tripled(left, s_v[...])
    start[1].wait()
    step = scal[0:1, 0:1]
    ratio = scal[1:2, 0:1]
    stores = []
    for tau in range(2):
        t = slice(tau * 16, tau * 16 + 16)
        for copy in halves[tau]:
            copy.wait()

        def body(i, carry):
            h = i * 2
            parts = []
            for j in range(2):
                parts.append(
                    jnp.concatenate(
                        [back[pl.ds(k * 12 + tau * 6 + h + j, 128, stride=ROWS), :] for k in range(3)], axis=0
                    )
                )
            out = dot(left[...], stacked(jnp.concatenate(parts, axis=1))).T
            for j in range(2):
                x = pl.ds(pl.multiple_of((h + j) * 8, 8), 8)
                d = d_v[t, x, :]
                nd_v[t, x, :] = out[j * 128 : (j + 1) * 128, :].reshape(16, 8, 384) + ratio.reshape(1, 1, 1) * d
                ns_v[t, x, :] = sol_v[t, x, :] + step.reshape(1, 1, 1) * d
                nr_v[t, x, :] = r_v[t, x, :] - step.reshape(1, 1, 1) * img_v[t, x, :]
            return carry

        lax.fori_loop(0, 3, body, 0)
        for n, (src, dst) in enumerate(((ns_v, new_sol), (nr_v, new_res), (nd_v, new_dir))):
            stores.append(pltpu.make_async_copy(src.at[t], dst.at[t], out_sem.at[tau * 3 + n]))
            stores[-1].start()
    for store in stores:
        store.wait()


VMEM = pl.BlockSpec(memory_space=pltpu.VMEM)
HBM = pl.BlockSpec(memory_space=pltpu.HBM)
SMEM = pl.BlockSpec(memory_space=pltpu.SMEM)


def per_device(solution, residual, direction, reaction, time_bands, space_bands, time_basis, space_basis, time_eigen, space_eigen):
    block = (32, 48, 384)
    chunks = (128 * ROWS, 128)
    v = pltpu.VMEM
    dma = pltpu.SemaphoreType.DMA
    image, back, scal = pl.pallas_call(
        main_kernel,
        out_shape=(
            jax.ShapeDtypeStruct(block, F32),
            jax.ShapeDtypeStruct(chunks, F32),
            jax.ShapeDtypeStruct((8, 128), F32),
        ),
        in_specs=[HBM] * 8 + [SMEM] * 2,
        out_specs=(HBM, HBM, VMEM),
        scratch_shapes=[
            v(block, F32), v((38, 64, 384), F32), v(block, F32), v(block, F32),
            v((384, 384), F32), v((3, 384, 128), F32), v((4, 512, 128), F32), v((2, 4, 384), F32),
            v((1, 512), F32), v((1, 384), F32), v((384, 512), F32),
            v((16, 384), F32), v((384, 16), F32), v((14, 48, 128), F32), v((384, 384), F32),
            v((384, 1152), BF16), v((384, 1152), BF16), v((384, 1152), BF16),
            v((512, 512), BF16), v((512, 512), BF16), v((1536, 1152), BF16),
            v(chunks, F32), v(chunks, F32), v(chunks, F32), v(chunks, F32),
            v((384, 512), F32), v((1152, 512), F32),
            v((38, 3, 64, 128), F32), v((38, 3, 64, 128), F32),
            v((38, 3, 48, 128), F32), v((38, 3, 48, 128), F32),
            v((2, 128), F32), v((256, 128), F32), v((1, 128), F32), v((128, 128), F32),
            pltpu.SMEM((448,), F32), dma((14,)), dma((8,)), dma((8,)), dma((2,)), dma((8,)), dma((8,)),
        ],
        compiler_params=pltpu.CompilerParams(
            collective_id=0, has_side_effects=True, vmem_limit_bytes=62 * 2**20
        ),
    )(
        residual, direction, reaction, space_basis, time_basis, space_bands,
        time_eigen.reshape(1, -1), space_eigen.reshape(1, -1), time_bands, space_eigen,
    )
    return pl.pallas_call(
        last_kernel,
        out_shape=(jax.ShapeDtypeStruct(block, F32),) * 3,
        in_specs=[HBM] * 6 + [VMEM],
        out_specs=(HBM,) * 3,
        scratch_shapes=[
            v(chunks, F32), v((384, 384), F32), v((384, 1152), BF16),
            *[v(block, F32) for _ in range(7)],
            dma((10,)), dma((6,)),
        ],
        compiler_params=pltpu.CompilerParams(vmem_limit_bytes=62 * 2**20),
    )(back, space_basis, direction, solution, residual, image, scal)


def solution(mesh):
    field = P("tm", "space", None)
    return jax.shard_map(
        per_device,
        mesh=mesh,
        in_specs=(field,) * 4 + (P(),) * 6,
        out_specs=(field,) * 3,
        check_vma=False,
    )
```

```python
import jax
import jax.numpy as jnp
from jax import lax
from jax.experimental import pallas as pl
from jax.experimental.pallas import tpu as pltpu
from jax.sharding import PartitionSpec as P

F32 = jnp.float32
BF16 = jnp.bfloat16
MESH = pl.DeviceIdType.MESH
ROWS = 36


def split(x):
    high = x.astype(BF16)
    return high, (x - high.astype(F32)).astype(BF16)


def dot(a, b, ca=1, cb=0):
    return lax.dot_general(a, b, (((ca,), (cb,)), ((), ())), preferred_element_type=F32)


def position():
    tm = lax.axis_index("tm")
    sp = lax.axis_index("space")
    return tm // 4, (tm // 2) % 2 * 2 + sp // 4, sp % 4, tm % 2


def device(z, x, y, c):
    return z * 4 + (x // 2) * 2 + c, (x % 2) * 4 + y


def wrapped(v):
    return jnp.where(v >= 4, v - 4, v)


def each_partner(where, act):
    z, x, y, c = where
    tops = [wrapped(z + a) * 4 for a in range(4)]
    cores = [c, 1 - c]

    def outer(b, carry):
        def inner(e, carry):
            xb = wrapped(x + b)
            yb = wrapped(wrapped(y + b) + e)
            for a in range(4):
                xa = wrapped(xb + a)
                high = jnp.where(xa >= 2, 2, 0)
                s = (xa - high) * 4 + wrapped(yb + a)
                for d in range(2):
                    t = tops[a] + high + cores[(a + d) % 2]
                    if a == 0 and d == 0:
                        pl.when(b + e > 0)(lambda: act(t, s))
                    else:
                        act(t, s)
            return carry

        return lax.fori_loop(0, 4, inner, carry)

    lax.fori_loop(0, 4, outer, 0)


def swap_lanes(pieces):
    lane = lax.broadcasted_iota(jnp.int32, (8, 128), 1)
    for bit in (1, 2, 4):
        low = (lane & bit) == 0
        moved = list(pieces)
        for p in range(8):
            if p & bit == 0:
                a, b = pieces[p], pieces[p | bit]
                moved[p] = jnp.where(low, a, pltpu.roll(b, bit, 1))
                moved[p | bit] = jnp.where(low, pltpu.roll(a, 128 - bit, 1), b)
        pieces = moved
    return pieces


def to_lines(chunks, k, lines):
    def body(h, carry):
        for tau in range(2):
            for top in range(2):
                row = k * 12 + tau * 6 + h
                got = [
                    chunks[pl.ds((top * 8 + p) * 8 * ROWS + row, 8, stride=ROWS), :]
                    for p in range(8)
                ]
                base = pl.multiple_of(h * 64, 64)
                lanes = slice((top * 2 + tau) * 128, (top * 2 + tau + 1) * 128)
                for x8, piece in enumerate(swap_lanes(got)):
                    lines[pl.ds(base + x8 * 8, 8), lanes] = piece
        return carry

    lax.fori_loop(0, 6, body, 0)


def to_chunks(lines, k, chunks):
    def body(h, carry):
        for tau in range(2):
            for top in range(2):
                row = k * 12 + tau * 6 + h
                base = pl.multiple_of(h * 64, 64)
                lanes = slice((top * 2 + tau) * 128, (top * 2 + tau + 1) * 128)
                got = [lines[pl.ds(base + x8 * 8, 8), lanes] for x8 in range(8)]
                for p, piece in enumerate(swap_lanes(got)):
                    chunks[pl.ds((top * 8 + p) * 8 * ROWS + row, 8, stride=ROWS), :] = piece
        return carry

    lax.fori_loop(0, 6, body, 0)


def pack_rows(field, packed):
    def body(i, carry):
        tau, h = i // 6, i % 6
        v = field[pl.ds(pl.multiple_of(tau * 16, 16), 16), pl.ds(pl.multiple_of(h * 8, 8), 8), :]
        high, low = split(v.reshape(128, 384))
        rows = pl.ds(pl.multiple_of(i * 128, 128), 128)
        packed[rows, 0:384] = high
        packed[rows, 384:768] = low
        packed[rows, 768:1152] = high
        return carry

    lax.fori_loop(0, 12, body, 0)


def forward_y(packed, left, chunks):
    def body(i, carry):
        out = dot(left[...], packed[pl.ds(pl.multiple_of(i * 256, 256), 256), :], 1, 1)
        for k in range(3):
            for j in range(2):
                chunks[pl.ds(k * 12 + i * 2 + j, 128, stride=ROWS), :] = out[
                    k * 128 : (k + 1) * 128, j * 128 : (j + 1) * 128
                ]
        return carry

    lax.fori_loop(0, 6, body, 0)


def tripled(ref, values):
    high, low = split(values)
    width = values.shape[1]
    ref[:, 0:width] = high
    ref[:, width : 2 * width] = high
    ref[:, 2 * width : 3 * width] = low


def stacked(values):
    high, low = split(values)
    return jnp.concatenate([high, low, high], axis=0)


def forward_tx(lines, time_high, time_low, left_x):
    high, low = split(lines[...])
    mid = dot(high, time_high[...]) + dot(high, time_low[...]) + dot(low, time_high[...])
    return dot(left_x[...], stacked(mid))


def send_all(where, copy_to):
    each_partner(where, lambda t, s: copy_to(t, s).start())


def stencil(ext, reac, ycoef, xcoef, tbands, first_t, tcoef, mass, stiff, mixed, rest, image):
    def time_weight(matrix, off, t):
        size = abs(off)
        if off <= 0:
            value = tbands[matrix, size, jnp.maximum(t - size, 0)]
            return jnp.where(t >= size, value, 0.0)
        return jnp.where(t + size < 512, tbands[matrix, size, t], 0.0)

    def along_y(t, carry):
        for part in range(2):
            rows = slice(part * 32, part * 32 + 32)
            v = ext[t, rows, :]
            m = ycoef[3:4, :] * v
            s = ycoef[10:11, :] * v
            for off in (-3, -2, -1, 1, 2, 3):
                moved = pltpu.roll(v, (-off) % 384, 1)
                m = m + ycoef[3 + off : 4 + off, :] * moved
                s = s + ycoef[10 + off : 11 + off, :] * moved
            for c in range(3):
                mass[t, c, rows, :] = m[:, c * 128 : (c + 1) * 128]
                stiff[t, c, rows, :] = s[:, c * 128 : (c + 1) * 128]
        return carry

    lax.fori_loop(0, 38, along_y, 0)

    for i in range(6):
        first = i * 8
        ms = [xcoef[j, first : first + 8, :] for j in range(7)]
        ks = [xcoef[7 + j, first : first + 8, :] for j in range(7)]

        def along_x(t, carry):
            for c in range(3):
                m = [mass[t, c, 5 + j + first : 13 + j + first, :] for j in range(7)]
                s = [stiff[t, c, 5 + j + first : 13 + j + first, :] for j in range(7)]
                a = ms[0] * m[0]
                b = ks[0] * m[0] + ms[0] * s[0]
                for j in range(1, 7):
                    a = a + ms[j] * m[j]
                    b = b + (ks[j] * m[j] + ms[j] * s[j])
                mixed[t, c, first : first + 8, :] = a
                rest[t, c, first : first + 8, :] = b
            return carry

        lax.fori_loop(0, 38, along_x, 0)

    def weights(t, carry):
        for j in range(7):
            tcoef[t * 14 + j] = time_weight(0, j - 3, first_t + t)
            tcoef[t * 14 + 7 + j] = time_weight(1, j - 3, first_t + t)
        return carry

    lax.fori_loop(0, 32, weights, 0)

    def along_t(pair, total):
        t = pair * 2
        kt = [[tcoef[(t + n) * 14 + j] for j in range(7)] for n in range(2)]
        mt = [[tcoef[(t + n) * 14 + 7 + j] for j in range(7)] for n in range(2)]
        for c in range(3):
            lanes = slice(c * 128, c * 128 + 128)
            for i in range(6):
                rows = slice(i * 8, i * 8 + 8)
                own = [ext[t + 3 + n, 8 + i * 8 : 16 + i * 8, lanes] for n in range(2)]
                value = [reac[t + n, rows, lanes] * own[n] for n in range(2)]
                for j in range(8):
                    a = mixed[t + j, c, rows, :]
                    b = rest[t + j, c, rows, :]
                    for n in range(2):
                        if 0 <= j - n < 7:
                            value[n] = value[n] + (kt[n][j - n] * a + mt[n][j - n] * b)
                for n in range(2):
                    image[t + n, rows, lanes] = value[n]
                    total = total + own[n] * value[n]
        return total

    return lax.fori_loop(0, 16, along_t, jnp.zeros((8, 128), F32))


def whole(x):
    return jnp.sum(jnp.sum(x, axis=1, keepdims=True), axis=0, keepdims=True)


def band_lines(table):
    lane = lax.broadcasted_iota(jnp.int32, (1, 384), 1)
    lines = []
    for off in range(-3, 4):
        size = abs(off)
        line = table[size : size + 1, :]
        if off < 0:
            line = jnp.where(lane >= size, pltpu.roll(line, size, 1), 0.0)
        elif off > 0:
            line = jnp.where(lane < 384 - size, line, 0.0)
        lines.append(line)
    return lines


def main_kernel(
    r_h, d_h, reac_h, s_h, t_h, sb_h, te_h, se_h, tbands, seig,
    img_h, back_h, scal_o,
    rv, ext, reac, image, s_v, s3, t4, sb_v, te_v, se_v, base_v, yc_v, xt_v, xc_v, sp_v,
    left_y, left_x, left_xi, time_high, time_low, packed,
    send1, send2, recv1, recv2, lines, hat_r,
    mass, stiff, mixed, rest, red1s, red1, red2s, red2,
    tcoef, local, halo_s, halo_r, out_sem, send_sem, recv_sem,
):
    where = position()
    tm = lax.axis_index("tm")
    sp = lax.axis_index("space")
    me = tm * 8 + sp
    pairs = [(d_h, ext.at[3:35, 8:56]), (s_h, s_v), (r_h, rv), (sb_h, sb_v), (reac_h, reac), (te_h, te_v), (se_h, se_v)]
    pairs += [(s_h.at[:, c * 128 : c * 128 + 128], s3.at[c]) for c in range(3)]
    pairs += [(t_h.at[:, c * 128 : c * 128 + 128], t4.at[c]) for c in range(4)]
    loads = [pltpu.make_async_copy(src, dst, local.at[n]) for n, (src, dst) in enumerate(pairs)]
    for load in loads:
        load.start()

    barrier = pltpu.get_barrier_semaphore()

    each_partner(
        where,
        lambda t, s: pl.semaphore_signal(barrier, inc=1, device_id=(t, s), device_id_type=MESH),
    )
    loads[1].wait()
    tripled(left_y, s_v[...].T)
    loads[2].wait()
    pack_rows(rv, packed)
    forward_y(packed, left_y, send1)
    loads[0].wait()
    pl.semaphore_wait(barrier, 127)

    halos = []
    for dt, src_t, dst_t in ((-1, slice(3, 6), slice(35, 38)), (0, slice(3, 35), slice(3, 35)), (1, slice(32, 35), slice(0, 3))):
        for dx, src_x, dst_x in ((-1, slice(8, 11), slice(56, 59)), (0, slice(8, 56), slice(8, 56)), (1, slice(53, 56), slice(5, 8))):
            if dt or dx:
                n = len(halos)
                halos.append(
                    pltpu.make_async_remote_copy(
                        src_ref=ext.at[src_t, src_x],
                        dst_ref=ext.at[dst_t, dst_x],
                        send_sem=halo_s.at[n],
                        recv_sem=halo_r.at[n],
                        device_id=((tm + 16 + dt) % 16, (sp + 8 + dx) % 8),
                        device_id_type=MESH,
                    )
                )
    for halo in halos:
        halo.start()

    def exchange(n, src, dst, start, rows):
        def copy_to(t, s):
            return pltpu.make_async_remote_copy(
                src_ref=src.at[pl.ds((t * 8 + s) * ROWS + start, rows)],
                dst_ref=dst.at[pl.ds(me * ROWS + start, rows)],
                send_sem=send_sem.at[n],
                recv_sem=recv_sem.at[n],
                device_id=(t, s),
                device_id_type=MESH,
            )

        send_all(where, copy_to)

    def finish(n, src, dst, rows):
        return pltpu.make_async_remote_copy(
            src_ref=src.at[pl.ds(0, 127 * rows)],
            dst_ref=dst.at[pl.ds(0, 127 * rows)],
            send_sem=send_sem.at[n],
            recv_sem=recv_sem.at[n],
            device_id=(tm, sp),
            device_id_type=MESH,
        )

    def own_chunk(src, dst):
        dst[pl.ds(me * ROWS, ROWS), :] = src[pl.ds(me * ROWS, ROWS), :]

    exchange(0, send1, recv1, 0, ROWS)
    own_chunk(send1, recv1)

    loads[3].wait()
    table = jnp.concatenate(band_lines(sb_v[1]) + band_lines(sb_v[0]) + [jnp.zeros((2, 384), F32)], axis=0)
    yc_v[...] = table
    xt_v[...] = table.T
    near = xt_v[pl.ds(pl.multiple_of(sp * 48, 16), 48), :]
    for j in range(14):
        xc_v[j] = jnp.broadcast_to(near[:, j : j + 1], (48, 128))
    for load in loads[4:]:
        load.wait()
    for halo in halos:
        halo.wait()
    curve = stencil(ext, reac, yc_v, xc_v, tbands, tm * 32, tcoef, mass, stiff, mixed, rest, image)
    store_image = pltpu.make_async_copy(image, img_h, out_sem.at[0])
    store_image.start()
    pack_rows(image, packed)

    forward_y(packed, left_y, send2)
    exchange(9, send2, recv2, 0, 12)
    exchange(10, send2, recv2, 12, 12)
    own_chunk(send2, recv2)

    for h in range(48):
        for c in range(3):
            sp_v[h * 8 : h * 8 + 8, c * 128 : c * 128 + 128] = s3[c, pl.ds(h, 8, stride=48), :]
    tripled(left_x, sp_v[...].T)
    tripled(left_xi, sp_v[...])

    def time_rows(i, carry):
        start = (i // 16) * 256 + (i // 8) % 2 * 16 + i % 8 * 2
        rows = pl.ds(pl.multiple_of(i * 16, 16), 16)
        for c in range(4):
            got = jnp.concatenate([t4[c, pl.ds(start + j, 8, stride=32), :] for j in range(2)], axis=0)
            high, low = split(got)
            time_high[rows, c * 128 : c * 128 + 128] = high
            time_low[rows, c * 128 : c * 128 + 128] = low
        return carry

    lax.fori_loop(0, 32, time_rows, 0)
    column = jnp.broadcast_to(se_v[...].reshape(1, 384), (8, 384)).T
    base_v[...] = column[:, 0:1] + te_v[...]

    def eigen(k):
        return base_v[...] + seig[k * 128 + me]

    def old_part(k, total):
        to_lines(recv1, k, lines)
        v = forward_tx(lines, time_high, time_low, left_x)
        hat_r[pl.ds(pl.multiple_of(k * 384, 384), 384), :] = v
        return total + jnp.sum((v * (v / eigen(k))).reshape(48, 8, 512), axis=0)

    finish(0, send1, recv1, ROWS).wait()
    old = lax.fori_loop(0, 3, old_part, jnp.zeros((8, 512), F32))
    old = old[:, 0:128] + old[:, 128:256] + old[:, 256:384] + old[:, 384:512]

    def share(n, mine, every, rows):
        def copy_to(t, s):
            return pltpu.make_async_remote_copy(
                src_ref=mine,
                dst_ref=every.at[pl.ds(me * rows, rows)],
                send_sem=send_sem.at[n],
                recv_sem=recv_sem.at[n],
                device_id=(t, s),
                device_id_type=MESH,
            )

        send_all(where, copy_to)
        every[pl.ds(me * rows, rows), :] = mine[...]

    red1s[0:1, :] = jnp.sum(old, axis=0, keepdims=True)
    red1s[1:2, :] = jnp.sum(curve, axis=0, keepdims=True)
    share(6, red1s, red1, 2)
    exchange(11, send2, recv2, 24, 12)

    finish(6, red1, red1, 2).wait()
    every = red1[...]
    even = lax.broadcasted_iota(jnp.int32, (256, 128), 0) % 2 == 0
    norm_old = whole(jnp.where(even, every, 0.0))
    step = norm_old / whole(jnp.where(even, 0.0, every))

    def inverse_part(k, total):
        finish(9 + k, send2, recv2, 12).wait()
        to_lines(recv2, k, lines)
        rows = pl.ds(pl.multiple_of(k * 384, 384), 384)
        v = hat_r[rows, :] - step * forward_tx(lines, time_high, time_low, left_x)
        g = v / eigen(k)
        high, low = split(dot(left_xi[...], stacked(g)))
        lines[...] = (
            dot(high, time_high[...], 1, 1)
            + dot(high, time_low[...], 1, 1)
            + dot(low, time_high[...], 1, 1)
        )
        to_chunks(lines, k, send1)
        exchange(3 + k, send1, back_h, k * 12, 12)
        return total + jnp.sum((v * g).reshape(48, 8, 512), axis=0)

    new = lax.fori_loop(0, 3, inverse_part, jnp.zeros((8, 512), F32))
    own = pltpu.make_async_copy(
        send1.at[pl.ds(me * ROWS, ROWS)], back_h.at[pl.ds(me * ROWS, ROWS)], out_sem.at[1]
    )
    own.start()

    new = new[:, 0:128] + new[:, 128:256] + new[:, 256:384] + new[:, 384:512]
    red2s[...] = jnp.sum(new, axis=0, keepdims=True)
    share(7, red2s, red2, 1)
    finish(7, red2, red2, 1).wait()
    norm_new = whole(red2[...])
    row = lax.broadcasted_iota(jnp.int32, (8, 128), 0)
    scal_o[...] = jnp.where(row == 0, step, norm_new / norm_old)

    store_image.wait()
    own.wait()
    for k in range(3):
        finish(3 + k, send1, back_h, 12).wait()


def last_kernel(
    back_h, s_h, d_h, sol_h, r_h, img_h, scal,
    new_sol, new_res, new_dir,
    back, s_v, left, d_v, sol_v, r_v, img_v, ns_v, nr_v, nd_v, in_sem, out_sem,
):
    start = [pltpu.make_async_copy(s_h, s_v, in_sem.at[0]), pltpu.make_async_copy(back_h, back, in_sem.at[1])]
    parts = [(slice(tau * 16, tau * 16 + 16), slice(i * 16, i * 16 + 16)) for tau in range(2) for i in range(3)]
    loads = [
        [
            pltpu.make_async_copy(src.at[t, x], dst.at[t, x], in_sem.at[2 + n * 4 + q])
            for q, (src, dst) in enumerate(((d_h, d_v), (sol_h, sol_v), (r_h, r_v), (img_h, img_v)))
        ]
        for n, (t, x) in enumerate(parts)
    ]
    for copy in start + sum(loads, []):
        copy.start()
    start[0].wait()
    tripled(left, s_v[...])
    step = scal[0:1, 0:1].reshape(1, 1, 1)
    ratio = scal[1:2, 0:1].reshape(1, 1, 1)
    start[1].wait()
    stores = []
    for n, (t, x) in enumerate(parts):
        lines = []
        for j in range(2):
            lines.append(
                jnp.concatenate([back[pl.ds(k * 12 + n * 2 + j, 128, stride=ROWS), :] for k in range(3)], axis=0)
            )
        out = dot(left[...], stacked(jnp.concatenate(lines, axis=1))).T
        for copy in loads[n]:
            copy.wait()
        ns_v[t, x, :] = sol_v[t, x, :] + step * d_v[t, x, :]
        nr_v[t, x, :] = r_v[t, x, :] - step * img_v[t, x, :]
        for j in range(2):
            part = slice(x.start + j * 8, x.start + j * 8 + 8)
            nd_v[t, part, :] = out[j * 128 : (j + 1) * 128, :].reshape(16, 8, 384) + ratio * d_v[t, part, :]
        for q, (src, dst) in enumerate(((ns_v, new_sol), (nr_v, new_res), (nd_v, new_dir))):
            stores.append(pltpu.make_async_copy(src.at[t, x], dst.at[t, x], out_sem.at[n * 3 + q]))
            stores[-1].start()
    for store in stores:
        store.wait()


VMEM = pl.BlockSpec(memory_space=pltpu.VMEM)
HBM = pl.BlockSpec(memory_space=pltpu.HBM)
SMEM = pl.BlockSpec(memory_space=pltpu.SMEM)


def per_device(solution, residual, direction, reaction, time_bands, space_bands, time_basis, space_basis, time_eigen, space_eigen):
    block = (32, 48, 384)
    chunks = (128 * ROWS, 128)
    v = pltpu.VMEM
    dma = pltpu.SemaphoreType.DMA
    image, back, scal = pl.pallas_call(
        main_kernel,
        out_shape=(
            jax.ShapeDtypeStruct(block, F32),
            jax.ShapeDtypeStruct(chunks, F32),
            jax.ShapeDtypeStruct((8, 128), F32),
        ),
        in_specs=[HBM] * 8 + [SMEM] * 2,
        out_specs=(HBM, HBM, VMEM),
        scratch_shapes=[
            v(block, F32), v((38, 64, 384), F32), v(block, F32), v(block, F32),
            v((384, 384), F32), v((3, 384, 128), F32), v((4, 512, 128), F32), v((2, 4, 384), F32),
            v((1, 512), F32), v((384,), F32), v((384, 512), F32),
            v((16, 384), F32), v((384, 16), F32), v((14, 48, 128), F32), v((384, 384), F32),
            v((384, 1152), BF16), v((384, 1152), BF16), v((384, 1152), BF16),
            v((512, 512), BF16), v((512, 512), BF16), v((1536, 1152), BF16),
            v(chunks, F32), v(chunks, F32), v(chunks, F32), v(chunks, F32),
            v((384, 512), F32), v((1152, 512), F32),
            v((38, 3, 64, 128), F32), v((38, 3, 64, 128), F32),
            v((38, 3, 48, 128), F32), v((38, 3, 48, 128), F32),
            v((2, 128), F32), v((256, 128), F32), v((1, 128), F32), v((128, 128), F32),
            pltpu.SMEM((448,), F32), dma((14,)), dma((8,)), dma((8,)), dma((2,)), dma((12,)), dma((12,)),
        ],
        compiler_params=pltpu.CompilerParams(
            collective_id=0, has_side_effects=True, vmem_limit_bytes=62 * 2**20
        ),
    )(
        residual, direction, reaction, space_basis, time_basis, space_bands,
        time_eigen.reshape(1, -1), space_eigen, time_bands, space_eigen,
    )
    return pl.pallas_call(
        last_kernel,
        out_shape=(jax.ShapeDtypeStruct(block, F32),) * 3,
        in_specs=[HBM] * 6 + [VMEM],
        out_specs=(HBM,) * 3,
        scratch_shapes=[
            v(chunks, F32), v((384, 384), F32), v((384, 1152), BF16),
            *[v(block, F32) for _ in range(7)],
            dma((26,)), dma((18,)),
        ],
        compiler_params=pltpu.CompilerParams(vmem_limit_bytes=62 * 2**20),
    )(back, space_basis, direction, solution, residual, image, scal)


def solution(mesh):
    field = P("tm", "space", None)
    return jax.shard_map(
        per_device,
        mesh=mesh,
        in_specs=(field,) * 4 + (P(),) * 6,
        out_specs=(field,) * 3,
        check_vma=False,
    )
```
